32 devices in a mesh: rep: 2 (over y), shard: 16 (over z, x, core).
Axes of the slice: x: 2, y: 2, z: 4, core: 2. Of those that a mesh axis runs over, the one named last changes fastest.
Arguments:
- row_ids: int32 [2, 16, 16, 128], P('rep', 'shard'), may hold values from -1 to 163839, as said below
- grad_rows: bfloat16 [2, 16, 16, 128, 128], P('rep', 'shard'), may hold values from -6 to 6
- touched: int32 [16, 20], P('shard'), may hold values from 0 to 39, as said below
- block_home: int32 [640], replicated, may hold values from 0 to 639, as said below
- embed_table: float32 [163840, 128], P('shard'), may hold values from -4 to 4
- row_accum: float32 [163840], P('shard'), may hold values from 0.001 to 0.1
Outputs:
- new_table: float32 [163840, 128], P('shard')
- new_accum: float32 [163840], P('shard')
The draws below stay inside these ranges and needn't reach their ends.
Inputs may be any that keep to these rules, and one draw needn't show every extreme that they name: block_home is a permutation of 0 to 639. Each row of touched holds 20 different local block numbers. `row_ids`: A live slot in bucket d of any device names a logical row whose stored row lies on index d of shard, in a local block listed in row d of touched; about three quarters of the slots are live.
All inputs are finite; a program needn't handle non-finite values.
Results may differ from the reference program's by a relative error of at most 0.0003.
Values may be sent and summed in bfloat16 or wider, within the bound.
No kernel may reach another device: no remote copies, remote signals or barrier semaphores. Data moves between devices by JAX's collectives and lax.ppermute only.
A program may use at most 64 MiB of HBM per device.

```python
import math
import jax
import jax.numpy as jnp
from jax import lax

E = 128
BLOCK = 256
BLK_DEV = 40
TOUCH = 20
SLOT = 128
BLOCKS = 640
ROWS = 163840
N_REP = 2
N_SHARD = 16


def layout_tables(key):
    home_key = jax.random.fold_in(key, 11)
    touch_key = jax.random.fold_in(key, 12)
    home_of = jax.random.permutation(home_key, BLOCKS).astype(jnp.int32)
    shard_keys = jax.random.split(touch_key, N_SHARD)
    listed = jax.vmap(lambda each_key: jax.random.permutation(each_key, BLK_DEV)[:TOUCH])(shard_keys)
    return (home_of, listed.astype(jnp.int32))


def draw_block_home(key, part):
    return layout_tables(key)[0]


def draw_touched(key, part):
    return layout_tables(key)[1]


def draw_row_ids(key, part):
    home_of, listed = layout_tables(key)
    block_of_home = jnp.argsort(home_of, stable=True).astype(jnp.int32)
    base_key = jax.random.fold_in(key, 13)
    pick_key, within_key, live_key = jax.random.split(base_key, 3)
    shape = (N_REP, N_SHARD, N_SHARD, SLOT)
    picked = jax.random.randint(pick_key, shape, 0, TOUCH)
    within = jax.random.randint(within_key, shape, 0, BLOCK)
    is_live = jax.random.randint(live_key, shape, 0, 4) < 3
    target = jax.lax.broadcasted_iota(jnp.int32, shape, 2)
    local_block = listed[target, picked]
    logical = block_of_home[target * BLK_DEV + local_block]
    return jnp.where(is_live, logical * BLOCK + within, -1).astype(jnp.int32)


def draw_grad_rows(key, part):
    slot_ids = draw_row_ids(key, part)
    noise_key = jax.random.fold_in(key, 14)
    common_key = jax.random.fold_in(key, 15)
    shape = (N_REP, N_SHARD, N_SHARD, SLOT, E)
    safe_ids = jnp.maximum(slot_ids, 0).reshape(-1)
    shared = jax.vmap(lambda each_id: jax.random.normal(jax.random.fold_in(common_key, each_id), (E,), jnp.float32))(safe_ids)
    shared = jnp.clip(shared, -6.0, 6.0).reshape(shape)
    noise = jnp.clip(jax.random.normal(noise_key, shape, jnp.float32), -6.0, 6.0)
    weight_shared = 0.6
    return jnp.clip(noise + weight_shared * shared, -6.0, 6.0).astype(jnp.bfloat16)


def steps_of(own_key, extent, cuts, smallest, top_value):
    loudness = 1.0
    for dim, shards_of in cuts:
        heights = jax.random.uniform(jax.random.fold_in(jax.random.fold_in(own_key, 6), dim), (shards_of,), jnp.float32, smallest / len(cuts), top_value / len(cuts))
        loudness = loudness * jnp.repeat(jnp.exp(heights), extent[dim] // shards_of).reshape((-1,) + (1,) * (len(extent) - 1 - dim))
    return loudness


def centred(key, dims, deviation, most, cuts=(), kind=jnp.bfloat16):
    entries = deviation * jax.random.normal(key, dims, jnp.float32)
    if cuts:
        entries = entries * steps_of(key, dims, cuts, -0.22, 0.18)
    return jnp.clip(entries, -most, most).astype(kind)


def setup_inputs(seed: int = 0) -> dict:
    seeds = jax.random.split(jax.random.key(seed), 7)
    return {
        "row_ids": draw_row_ids(jax.random.fold_in(seeds[6], 71), 0),
        "grad_rows": draw_grad_rows(jax.random.fold_in(seeds[6], 71), 0),
        "touched": draw_touched(jax.random.fold_in(seeds[6], 71), 0),
        "block_home": draw_block_home(jax.random.fold_in(seeds[6], 71), 0),
        "embed_table": centred(seeds[4], (ROWS, E), 0.5, 4.0, ((0, 16),), jnp.float32),
        "row_accum": jnp.clip(jnp.exp(math.log(0.1) - 4.6051702 * jax.random.uniform(seeds[5], (ROWS,), jnp.float32) ** steps_of(seeds[5], (ROWS,), ((0, 16),), -0.2, 0.2)), 0.001, 0.1),
    }


CLIP_RMS = 0.25
LEARN_RATE = 0.1
DECAY_RATE = 0.05

def reference(row_ids, grad_rows, touched, block_home, embed_table, row_accum):
    sample_ids = row_ids.reshape(-1).astype(jnp.int32)
    gradients = grad_rows.reshape(-1, E).astype(jnp.float32)
    is_live = sample_ids >= 0
    safe_ids = jnp.where(is_live, sample_ids, 0)
    stored = block_home[safe_ids // BLOCK] * BLOCK + safe_ids % BLOCK
    stored = jnp.where(is_live, stored, ROWS).astype(jnp.int32)
    summed = jax.ops.segment_sum(gradients, stored, num_segments=ROWS + 1)[:ROWS]
    square_sum = jnp.sum(summed * summed)
    clip_limit = CLIP_RMS * (N_SHARD * TOUCH * BLOCK * E) ** 0.5
    clip_factor = clip_limit / jnp.maximum(jnp.sqrt(square_sum), clip_limit)
    scaled = summed * clip_factor
    new_accum = row_accum + lax.optimization_barrier(jnp.mean(scaled * scaled, axis=1))
    owners = jnp.arange(N_SHARD, dtype=jnp.int32)[:, None] * BLK_DEV
    touched_blocks = (owners + touched.astype(jnp.int32)).reshape(-1)
    block_mask = jnp.zeros((BLOCKS,), jnp.float32).at[touched_blocks].set(1.0)
    row_mask = jnp.repeat(block_mask, BLOCK)[:, None]
    decayed = embed_table * (1.0 - DECAY_RATE * row_mask)
    new_table = decayed - LEARN_RATE * scaled / jnp.sqrt(new_accum)[:, None]
    return (new_table, new_accum)
```

```python
import functools
import math

import jax
import jax.numpy as jnp
from jax import lax
from jax.experimental import pallas as pl
from jax.experimental.pallas import tpu as pltpu
from jax.sharding import PartitionSpec as P

BLOCK = 256
CLIP_RMS = 0.25
LEARN_RATE = 0.1
DECAY_RATE = 0.05
LANES = 128
META = 8
MIB = 1 << 20


VMEM = pl.BlockSpec(memory_space=pltpu.VMEM)
SMEM = pl.BlockSpec(memory_space=pltpu.SMEM)
ANY = pl.BlockSpec(memory_space=pl.ANY)


def params(mib):
    return pltpu.CompilerParams(vmem_limit_bytes=mib * MIB)


def cost(us, bytes_accessed=MIB):
    return pl.CostEstimate(
        flops=int(us * 4e6), bytes_accessed=bytes_accessed, transcendentals=0
    )


def lane_pad(ids):
    pad = LANES - ids.shape[-1]
    return jnp.pad(ids, ((0, 0), (0, pad)), constant_values=-1) if pad else ids


def pack_kernel(half, ids_ref, grads_ref, first_ref, second_ref, sems):
    groups = ids_ref.shape[0]
    copy_a = pltpu.make_async_copy(
        grads_ref.at[:, pl.ds(0, half), :], first_ref.at[:, pl.ds(0, half), :], sems.at[0]
    )
    copy_b = pltpu.make_async_copy(
        grads_ref.at[:, pl.ds(half, half), :], second_ref, sems.at[1]
    )
    copy_a.start()
    copy_b.start()
    row = lax.broadcasted_iota(jnp.int32, (META, LANES), 0)
    for group in range(groups):
        ids = jnp.broadcast_to(ids_ref[group : group + 1, :], (META, LANES))
        live = ids >= 0
        top = jnp.where(live, ids >> 16, -1)
        digits = jnp.where(
            row == 0, top, jnp.where(row == 1, (ids >> 8) & 255, ids & 255)
        )
        first_ref[group, half : half + META, :] = digits.astype(jnp.float32).astype(
            jnp.bfloat16
        )
    copy_a.wait()
    copy_b.wait()


def pack(ids, grads):
    groups, slots, width = grads.shape
    half = slots // 2
    return pl.pallas_call(
        functools.partial(pack_kernel, half),
        out_shape=(
            jax.ShapeDtypeStruct((groups, half + META, width), grads.dtype),
            jax.ShapeDtypeStruct((groups, half, width), grads.dtype),
        ),
        in_specs=[VMEM, ANY],
        out_specs=(VMEM, VMEM),
        scratch_shapes=[pltpu.SemaphoreType.DMA((2,))],
        compiler_params=params(8),
        cost_estimate=cost(1.5),
        name="pack",
    )(ids, grads)


def table_kernel(
    touched_ref, table_ref, accum_ref, out_ref, old_ref, rep_ref, bounce, other, sems
):
    blocks, touch = table_ref.shape[0], touched_ref.shape[0]

    def clear(b, _):
        other[b] = 0
        return 0

    lax.fori_loop(0, blocks, clear, 0)

    def fetch(t, _):
        b = touched_ref[t]
        other[b] = 1
        pltpu.make_async_copy(table_ref.at[b], old_ref.at[t], sems.at[0]).start()
        return 0

    lax.fori_loop(0, touch, fetch, 0)

    def fetch_other(b, count):
        free = other[b] == 0

        @pl.when(free)
        def _():
            pltpu.make_async_copy(table_ref.at[b], bounce.at[count], sems.at[1]).start()
            other[blocks + count] = b

        return count + free.astype(jnp.int32)

    lax.fori_loop(0, blocks, fetch_other, 0)
    pltpu.make_async_copy(bounce, bounce, sems.at[1]).wait()

    def put(j, _):
        b = other[blocks + j]
        pltpu.make_async_copy(bounce.at[j], out_ref.at[b], sems.at[2]).start()
        return 0

    lax.fori_loop(0, blocks - touch, put, 0)

    def spread(t, _):
        b = touched_ref[t]
        for part in range(BLOCK // LANES):
            row = accum_ref[pl.ds(b * (BLOCK // LANES) + part, 1), :]
            rep_ref[t, part * LANES : (part + 1) * LANES, :] = jnp.broadcast_to(
                row, (LANES, LANES)
            ).T
        return 0

    lax.fori_loop(0, touch, spread, 0)
    pltpu.make_async_copy(old_ref, old_ref, sems.at[0]).wait()
    pltpu.make_async_copy(bounce, bounce, sems.at[2]).wait()


def split_table(touched, table, accum):
    blocks, touch = table.shape[0], touched.shape[0]
    width = table.shape[2]
    return pl.pallas_call(
        table_kernel,
        out_shape=(
            jax.ShapeDtypeStruct(table.shape, table.dtype),
            jax.ShapeDtypeStruct((touch, BLOCK, width), table.dtype),
            jax.ShapeDtypeStruct((touch, BLOCK, LANES), jnp.float32),
        ),
        in_specs=[SMEM, ANY, VMEM],
        out_specs=(ANY, VMEM, VMEM),
        scratch_shapes=[
            pltpu.VMEM((blocks - touch, BLOCK, width), table.dtype),
            pltpu.SMEM((2 * blocks,), jnp.int32),
            pltpu.SemaphoreType.DMA((3,)),
        ],
        compiler_params=params(16),
        cost_estimate=cost(4.0, 8 * MIB),
        name="split_table",
    )(touched, table, accum)


def slot_keys(home_ref, first_ref, half):
    groups = first_ref.shape[0]
    per = LANES // half
    lane = lax.broadcasted_iota(jnp.int32, (1, LANES), 1)
    rows = home_ref.shape[0]
    meta = first_ref[:, half : half + META, :].astype(jnp.float32)
    top, mid, low = (meta[:, i, :].astype(jnp.int32) for i in range(3))
    block = top * 256 + mid
    lo, hi = block & (LANES - 1), block >> 7
    home = jnp.zeros_like(block)
    for r in range(rows):
        line = jnp.broadcast_to(home_ref[r : r + 1, :], block.shape)
        found = jnp.take_along_axis(line, lo, axis=1)
        home = jnp.where(hi == r, found, home)
    keys = jnp.where(top >= 0, home * BLOCK + low, -1)
    firsts, seconds = [], []
    for g in range(groups // per):
        a = b = None
        for j in range(per):
            key = keys[g * per + j : g * per + j + 1, :]
            inside = (lane >= j * half) & (lane < (j + 1) * half)
            one = pltpu.roll(key, j * half, 1) if j else key
            two = pltpu.roll(key, (j * half - half) % LANES, 1) if j != 1 else key
            a = one if a is None else jnp.where(inside, one, a)
            b = two if b is None else jnp.where(inside, two, b)
        firsts.append(a)
        seconds.append(b)
    return firsts, seconds


def add_products(base, touched_ref, keys_ref, data_ref, half, sums_ref, fresh, visit):
    tile = 2 * LANES
    per = tile // half
    tiles = data_ref.shape[0] // per
    touch = touched_ref.shape[0]
    row = lax.broadcasted_iota(jnp.int32, (BLOCK, tile), 0)

    def step(t, carry):
        start = (base + touched_ref[t]) * BLOCK
        total = None if fresh else sums_ref[t]
        for k in range(tiles):
            keys = jnp.concatenate(
                [keys_ref[2 * k : 2 * k + 1, :], keys_ref[2 * k + 1 : 2 * k + 2, :]], axis=1
            )
            match = row == jnp.broadcast_to(keys - start, (BLOCK, tile))
            onehot = jnp.where(match, 1.0, 0.0).astype(jnp.bfloat16)
            rows = data_ref[k * per : (k + 1) * per, 0:half, :].reshape(tile, -1)
            part = jnp.dot(onehot, rows, preferred_element_type=jnp.float32)
            total = part if total is None else total + part
        sums_ref[t] = total
        return visit(total, carry)

    return step, touch


def first_kernel(half, fresh, base_ref, touched_ref, home_ref, data_ref, *rest):
    sums_ref, second_ref, keys = rest[-3:]
    if not fresh:
        sums_ref = rest[-3]
    firsts, seconds = slot_keys(home_ref, data_ref, half)
    for g, key in enumerate(firsts):
        keys[g : g + 1, :] = key
    for g, key in enumerate(seconds):
        second_ref[g : g + 1, :] = key
    step, touch = add_products(
        base_ref[0], touched_ref, keys, data_ref, half, sums_ref, fresh, lambda s, c: c
    )
    lax.fori_loop(0, touch, step, 0)


def second_kernel(half, base_ref, touched_ref, keys_ref, data_ref, sums_in, sums_ref):
    step, touch = add_products(
        base_ref[0], touched_ref, keys_ref, data_ref, half, sums_ref, False, lambda s, c: c
    )
    lax.fori_loop(0, touch, step, 0)


def last_kernel(half, base_ref, touched_ref, keys_ref, data_ref, sums_in, sums_ref, sq_ref):
    def visit(total, carry):
        square = (total * total).reshape(-1, 8, total.shape[-1])
        return carry + jnp.sum(square, axis=0)

    step, touch = add_products(
        base_ref[0], touched_ref, keys_ref, data_ref, half, sums_ref, False, visit
    )
    square = lax.fori_loop(0, touch, step, jnp.zeros((8, data_ref.shape[-1]), jnp.float32))
    for g in range(sq_ref.shape[0]):
        sq_ref[g] = square


def sums_first(base, touched, home, data, half, sums=None):
    touch = touched.shape[0]
    groups, _, width = data.shape
    key_rows = groups * half // LANES
    fresh = sums is None
    return pl.pallas_call(
        functools.partial(first_kernel, half, fresh),
        out_shape=(
            jax.ShapeDtypeStruct((touch, BLOCK, width), jnp.float32),
            jax.ShapeDtypeStruct((key_rows, LANES), jnp.int32),
        ),
        in_specs=[SMEM, SMEM, VMEM, VMEM] + ([] if fresh else [VMEM]),
        out_specs=(VMEM, VMEM),
        scratch_shapes=[pltpu.VMEM((key_rows, LANES), jnp.int32)],
        input_output_aliases={} if fresh else {4: 0},
        compiler_params=params(12),
        cost_estimate=cost(3.0),
        name="sums_first",
    )(base, touched, home, data, *([] if fresh else [sums]))


def sums_second(base, touched, keys, data, half, sums):
    return pl.pallas_call(
        functools.partial(second_kernel, half),
        out_shape=jax.ShapeDtypeStruct(sums.shape, jnp.float32),
        in_specs=[SMEM, SMEM, VMEM, VMEM, VMEM],
        out_specs=VMEM,
        input_output_aliases={4: 0},
        compiler_params=params(12),
        cost_estimate=cost(3.0),
        name="sums_second",
    )(base, touched, keys, data, sums)


def sums_last(base, touched, keys, data, half, sums, shards):
    return pl.pallas_call(
        functools.partial(last_kernel, half),
        out_shape=(
            jax.ShapeDtypeStruct(sums.shape, jnp.float32),
            jax.ShapeDtypeStruct((shards, 8, data.shape[-1]), jnp.float32),
        ),
        in_specs=[SMEM, SMEM, VMEM, VMEM, VMEM],
        out_specs=(VMEM, VMEM),
        input_output_aliases={4: 0},
        compiler_params=params(12),
        cost_estimate=cost(3.0),
        name="sums_last",
    )(base, touched, keys, data, sums)


def rows_kernel(touched_ref, sums_ref, rep_ref, flat_ref):
    width = sums_ref.shape[-1]
    flat_ref[...] = jnp.zeros_like(flat_ref)
    parts = BLOCK // LANES

    def step(t, _):
        total = sums_ref[t]
        square = total * total * (1.0 / width)
        mean = jnp.sum(square, axis=1, keepdims=True)
        wide = jnp.broadcast_to(mean, (BLOCK, LANES))
        rep_ref[t] = wide
        b = touched_ref[t]
        for part in range(parts):
            line = wide[part * LANES : (part + 1) * LANES, :].T
            flat_ref[pl.ds(b * parts + part, 1), :] = line[0:1, :]
        return 0

    lax.fori_loop(0, touched_ref.shape[0], step, 0)


def row_means(touched, sums, accum_rows):
    touch = touched.shape[0]
    return pl.pallas_call(
        rows_kernel,
        out_shape=(
            jax.ShapeDtypeStruct((touch, BLOCK, LANES), jnp.float32),
            jax.ShapeDtypeStruct((accum_rows, LANES), jnp.float32),
        ),
        in_specs=[SMEM, VMEM],
        out_specs=(VMEM, VMEM),
        compiler_params=params(12),
        cost_estimate=cost(2.0),
        name="row_means",
    )(touched, sums)


def update_kernel(
    limit, touched_ref, square_ref, sums_ref, old_ref, accum_rep_ref, mean_rep_ref,
    accum_ref, mean_ref, table_in, table_ref, new_accum_ref, fresh, sem,
):
    square = jnp.sum(square_ref[...], axis=0)
    square = jnp.sum(jnp.sum(square, axis=1, keepdims=True), axis=0, keepdims=True)
    factor = limit / jnp.maximum(jnp.sqrt(square), limit)
    factor_sq = factor * factor
    new_accum_ref[...] = accum_ref[...] + factor_sq * mean_ref[...]
    rate = LEARN_RATE * factor

    def step(t, _):
        accum = accum_rep_ref[t] + factor_sq * mean_rep_ref[t]
        fresh[t] = old_ref[t] * (1.0 - DECAY_RATE) - (rate * sums_ref[t]) * lax.rsqrt(accum)
        pltpu.make_async_copy(fresh.at[t], table_ref.at[touched_ref[t]], sem).start()
        return 0

    lax.fori_loop(0, touched_ref.shape[0], step, 0)
    pltpu.make_async_copy(fresh, fresh, sem).wait()


def update(limit, touched, square, sums, old, accum_rep, mean_rep, accum, mean, table):
    return pl.pallas_call(
        functools.partial(update_kernel, limit),
        out_shape=(
            jax.ShapeDtypeStruct(table.shape, table.dtype),
            jax.ShapeDtypeStruct(accum.shape, accum.dtype),
        ),
        in_specs=[SMEM] + [VMEM] * 7 + [ANY],
        out_specs=(ANY, VMEM),
        scratch_shapes=[pltpu.VMEM(old.shape, old.dtype), pltpu.SemaphoreType.DMA],
        input_output_aliases={8: 0},
        compiler_params=params(20),
        cost_estimate=cost(2.5),
        name="update",
    )(touched, square, sums, old, accum_rep, mean_rep, accum, mean, table)


def body(row_ids, grad_rows, touched, block_home, embed_table, row_accum):
    shards, slots, width = grad_rows.shape[2:]
    half = slots // 2
    blocks_here = embed_table.shape[0] // BLOCK
    listed = touched[0]
    touch = listed.shape[0]
    limit = CLIP_RMS * math.sqrt(lax.axis_size("shard") * touch * BLOCK * width)
    reps = lax.axis_size("rep")
    swap = [(i, (i + 1) % reps) for i in range(reps)]

    def exchange(x):
        return lax.all_to_all(x, "shard", 0, 0, tiled=True)

    first, second = pack(lane_pad(row_ids[0, 0]), grad_rows[0, 0])
    table = embed_table.reshape(blocks_here, BLOCK, width)
    accum = row_accum.reshape(-1, LANES)
    home = jnp.pad(block_home, (0, -block_home.shape[0] % LANES)).reshape(-1, LANES)
    base = (lax.axis_index("shard") * blocks_here).astype(jnp.int32).reshape(1)
    first, second = exchange(first), exchange(second)
    table_out, old, accum_rep = split_table(listed, table, accum)

    sums, keys = sums_first(base, listed, home, first, half)
    other_first = lax.ppermute(first, "rep", swap)
    other_second = lax.ppermute(second, "rep", swap)
    sums = sums_second(base, listed, keys, second, half, sums)
    sums, other_keys = sums_first(base, listed, home, other_first, half, sums)
    sums, square = sums_last(base, listed, other_keys, other_second, half, sums, shards)
    square = exchange(square)
    mean_rep, mean = row_means(listed, sums, accum.shape[0])
    table_out, accum_out = update(
        limit, listed, square, sums, old, accum_rep, mean_rep, accum, mean, table_out
    )
    return table_out.reshape(-1, width), accum_out.reshape(-1)


def solution(mesh):
    assert mesh.shape["rep"] == 2
    in_specs = (
        P("rep", "shard", None, None),
        P("rep", "shard", None, None, None),
        P("shard", None),
        P(),
        P("shard", None),
        P("shard"),
    )
    out_specs = (P("shard", None), P("shard"))
    return jax.shard_map(body, mesh=mesh, in_specs=in_specs, out_specs=out_specs, check_vma=False)
```

```python
import functools
import math

import jax
import jax.numpy as jnp
from jax import lax
from jax.experimental import pallas as pl
from jax.experimental.pallas import tpu as pltpu
from jax.sharding import PartitionSpec as P

BLOCK = 256
CLIP_RMS = 0.25
LEARN_RATE = 0.1
DECAY_RATE = 0.05
LANES = 128
META = 8
PARTS = BLOCK // LANES
TILE = 2 * LANES
MIB = 1 << 20
WHOLE = 67043328


VMEM = pl.BlockSpec(memory_space=pltpu.VMEM)
HBM = pl.BlockSpec(memory_space=pltpu.HBM)


def call(kernel, us, mib, **kwargs):
    return pl.pallas_call(
        kernel,
        compiler_params=pltpu.CompilerParams(vmem_limit_bytes=int(min(mib * MIB, WHOLE))),
        cost_estimate=pl.CostEstimate(
            flops=int(us * 4e6), bytes_accessed=MIB, transcendentals=0
        ),
        **kwargs,
    )


def like(shape, dtype=jnp.float32):
    return jax.ShapeDtypeStruct(shape, dtype)


def pack_kernel(slots, ids_hbm, grads_hbm, out_ref, ids_ref, sems):
    groups = ids_ref.shape[0]
    fetch = pltpu.make_async_copy(ids_hbm, ids_ref, sems.at[0])
    copy = pltpu.make_async_copy(grads_hbm, out_ref.at[:, pl.ds(0, slots), :], sems.at[1])
    fetch.start()
    copy.start()
    row = lax.broadcasted_iota(jnp.int32, (META, LANES), 0)
    fetch.wait()
    for group in range(groups):
        ids = jnp.broadcast_to(ids_ref[group : group + 1, :], (META, LANES))
        top = jnp.where(ids >= 0, ids >> 16, -1)
        digits = jnp.where(
            row == 0, top, jnp.where(row == 1, (ids >> 8) & 255, ids & 255)
        )
        out_ref[group, slots : slots + META, :] = digits.astype(jnp.float32).astype(
            jnp.bfloat16
        )
    copy.wait()


def pack(ids, grads):
    groups, slots, width = grads.shape
    pad = LANES - slots
    ids = jnp.pad(ids, ((0, 0), (0, pad)), constant_values=-1) if pad else ids
    return call(
        functools.partial(pack_kernel, slots),
        1.0,
        64,
        out_shape=like((groups, slots + META, width), grads.dtype),
        in_specs=[HBM, HBM],
        out_specs=VMEM,
        scratch_shapes=[
            pltpu.VMEM((groups, LANES), jnp.int32),
            pltpu.SemaphoreType.DMA((2,)),
        ],
    )(ids, grads)


def keep_kernel(touched_hbm, table_hbm, out_hbm, listed, bounce, other, sems):
    blocks, touch = table_hbm.shape[0], touched_hbm.shape[1]
    fetch = pltpu.make_async_copy(touched_hbm, listed, sems.at[0])
    fetch.start()

    def clear(b, _):
        other[b] = 0
        return 0

    lax.fori_loop(0, blocks, clear, 0)
    fetch.wait()

    def mark(t, _):
        other[listed[0, t]] = 1
        return 0

    lax.fori_loop(0, touch, mark, 0)

    def pull(b, count):
        free = other[b] == 0

        @pl.when(free)
        def _():
            pltpu.make_async_copy(table_hbm.at[b], bounce.at[count], sems.at[1]).start()
            other[blocks + count] = b

        return count + free.astype(jnp.int32)

    lax.fori_loop(0, blocks, pull, 0)
    pltpu.make_async_copy(bounce, bounce, sems.at[1]).wait()

    def put(j, _):
        b = other[blocks + j]
        pltpu.make_async_copy(bounce.at[j], out_hbm.at[b], sems.at[2]).start()
        return 0

    lax.fori_loop(0, blocks - touch, put, 0)
    pltpu.make_async_copy(bounce, bounce, sems.at[2]).wait()


def keep_untouched(touched, table):
    blocks, _, width = table.shape
    touch = touched.shape[1]
    return call(
        keep_kernel,
        4.0,
        64,
        out_shape=like(table.shape, table.dtype),
        in_specs=[HBM, HBM],
        out_specs=HBM,
        scratch_shapes=[
            pltpu.SMEM((1, touch), jnp.int32),
            pltpu.VMEM((blocks - touch, BLOCK, width), table.dtype),
            pltpu.SMEM((2 * blocks,), jnp.int32),
            pltpu.SemaphoreType.DMA((3,)),
        ],
    )(touched, table)


def keys_kernel(slots, blocks_here, touched_hbm, home_hbm, data_ref, keys_ref, listed, home_ref, sems):
    a = pltpu.make_async_copy(touched_hbm, listed, sems.at[0])
    b = pltpu.make_async_copy(home_hbm, home_ref, sems.at[1])
    a.start()
    b.start()
    groups, touch = data_ref.shape[0], listed.shape[1]
    per = LANES // slots
    lane = lax.broadcasted_iota(jnp.int32, (1, LANES), 1)
    meta = data_ref[:, slots : slots + META, :].astype(jnp.float32)
    top, mid, low = (meta[:, i, :].astype(jnp.int32) for i in range(3))
    block = top * 256 + mid
    lo, hi = block & (LANES - 1), block >> 7
    home = jnp.zeros_like(block)
    a.wait()
    b.wait()
    for r in range(home_ref.shape[0]):
        line = jnp.broadcast_to(home_ref[r : r + 1, :], block.shape)
        found = jnp.take_along_axis(line, lo, axis=1)
        home = jnp.where(hi == r, found, home)
    local = jnp.where(top >= 0, home - lax.axis_index("shard") * blocks_here, -1)
    keys = jnp.full_like(block, -1)
    for t in range(touch):
        keys = jnp.where(local == listed[0, t], t * BLOCK + low, keys)
    if per == 1:
        keys_ref[...] = keys
        return
    for g in range(groups // per):
        line = keys[g * per : g * per + 1, :]
        for j in range(1, per):
            key = pltpu.roll(keys[g * per + j : g * per + j + 1, :], j * slots, 1)
            line = jnp.where((lane >= j * slots) & (lane < (j + 1) * slots), key, line)
        keys_ref[g : g + 1, :] = line


def slot_keys(touched, home, data, slots, blocks_here):
    groups = data.shape[0]
    return call(
        functools.partial(keys_kernel, slots, blocks_here),
        1.0,
        4,
        out_shape=like((groups * slots // LANES, LANES), jnp.int32),
        in_specs=[HBM, HBM, VMEM],
        out_specs=VMEM,
        scratch_shapes=[
            pltpu.SMEM(touched.shape, jnp.int32),
            pltpu.VMEM(home.shape, jnp.int32),
            pltpu.SemaphoreType.DMA((2,)),
        ],
    )(touched, home, data)


def add_rows(slots, fresh, squared, first, keys_ref, data_ref, *refs):
    sums_ref, weights = refs[0 if fresh else 1], refs[-1]
    touch, _, width = sums_ref.shape
    per = TILE // slots
    tiles = data_ref.shape[0] // per
    many = next(m for m in (4, 2, 1) if touch % m == 0)
    key_rows = []
    for k in range(tiles):
        at = first + 2 * k
        pair = [keys_ref[at + i : at + i + 1, :] for i in range(2)]
        upper = [((key >> 7) & 1).astype(jnp.float32) for key in pair]
        upper = [jnp.broadcast_to(u, (LANES, LANES)).T for u in upper]
        upper = jnp.concatenate(upper, axis=0).astype(jnp.bfloat16)
        rows = data_ref[k * per : (k + 1) * per, 0:slots, :].reshape(TILE, width)
        high = rows * upper
        weights[k, :, width : 2 * width] = high
        weights[k, :, 0:width] = rows - high
        flat = [jnp.where(key >= 0, (key >> 8) * LANES + (key & (LANES - 1)), -1) for key in pair]
        key_rows.append(jnp.concatenate(flat, axis=1))
    row = lax.broadcasted_iota(jnp.int32, (many * LANES, TILE), 0)

    def step(u, carry):
        total = None
        for k in range(tiles):
            match = row == jnp.broadcast_to(key_rows[k] - u * (many * LANES), row.shape)
            onehot = jnp.where(match, 1.0, 0.0).astype(jnp.bfloat16)
            part = jnp.dot(onehot, weights[k], preferred_element_type=jnp.float32)
            total = part if total is None else total + part
        for i in range(many):
            t = u * many + i
            for p in range(PARTS):
                piece = total[i * LANES : (i + 1) * LANES, p * width : (p + 1) * width]
                at = pl.ds(p * LANES, LANES)
                piece = piece if fresh else piece + sums_ref[t, at, :]
                sums_ref[t, at, :] = piece
                if squared:
                    carry = carry + jnp.sum((piece * piece).reshape(-1, 8, width), axis=0)
        return carry

    carry = jnp.zeros((8, width), jnp.float32) if squared else 0
    carry = lax.fori_loop(0, touch // many, step, carry)
    if squared:
        refs[-2][...] = carry


def sums_of(keys, data, slots, touch, first=0, sums=None, squared=False):
    width = data.shape[-1]
    fresh = sums is None
    return call(
        functools.partial(add_rows, slots, fresh, squared, first),
        data.shape[0] * slots / 512,
        10,
        out_shape=(like((touch, BLOCK, width)), like((8, width)))[: 1 + squared],
        in_specs=[VMEM] * (2 if fresh else 3),
        out_specs=(VMEM, VMEM)[: 1 + squared],
        scratch_shapes=[
            pltpu.VMEM((data.shape[0] * slots // TILE, TILE, 2 * width), data.dtype)
        ],
        input_output_aliases={} if fresh else {2: 0},
    )(keys, data, *([] if fresh else [sums]))


def spread_kernel(touched_hbm, accum_hbm, rep_ref, listed, accum, sems):
    a = pltpu.make_async_copy(touched_hbm, listed, sems.at[0])
    b = pltpu.make_async_copy(accum_hbm, accum, sems.at[1])
    a.start()
    b.start()
    a.wait()
    b.wait()

    def step(t, _):
        for part in range(PARTS):
            row = accum[pl.ds(listed[0, t] * PARTS + part, 1), :]
            rep_ref[t, part * LANES : (part + 1) * LANES, :] = jnp.broadcast_to(
                row, (LANES, LANES)
            ).T
        return 0

    lax.fori_loop(0, rep_ref.shape[0], step, 0)


def spread_accum(touched, accum):
    touch = touched.shape[1]
    return call(
        spread_kernel,
        2.0,
        8,
        out_shape=like((touch, BLOCK, LANES)),
        in_specs=[HBM, HBM],
        out_specs=VMEM,
        scratch_shapes=[
            pltpu.SMEM((1, touch), jnp.int32),
            pltpu.VMEM(accum.shape, accum.dtype),
            pltpu.SemaphoreType.DMA((2,)),
        ],
    )(touched, accum)


def means_kernel(touched_hbm, sums_ref, rep_ref, flat_ref, listed, turned, sem):
    touch, _, width = sums_ref.shape
    fetch = pltpu.make_async_copy(touched_hbm, listed, sem)
    fetch.start()
    flat_ref[...] = jnp.zeros_like(flat_ref)
    lane = lax.broadcasted_iota(jnp.int32, (LANES, LANES), 1)

    def step(t, gathered):
        total = sums_ref[t]
        square = total * total * (1.0 / width)
        wide = jnp.broadcast_to(jnp.sum(square, axis=1, keepdims=True), (BLOCK, LANES))
        rep_ref[t] = wide
        for part in range(PARTS):
            piece = wide[part * LANES : (part + 1) * LANES, :]
            gathered = jnp.where(lane == t * PARTS + part, piece, gathered)
        return gathered

    gathered = lax.fori_loop(0, touch, step, jnp.zeros((LANES, LANES), jnp.float32))
    turned[...] = gathered.T
    fetch.wait()
    for t in range(touch):
        for part in range(PARTS):
            j = t * PARTS + part
            flat_ref[pl.ds(listed[0, t] * PARTS + part, 1), :] = turned[j : j + 1, :]


def row_means(touched, sums, accum_rows):
    touch = touched.shape[1]
    assert touch * PARTS <= LANES
    return call(
        means_kernel,
        2.0,
        8,
        out_shape=(like((touch, BLOCK, LANES)), like((accum_rows, LANES))),
        in_specs=[HBM, VMEM],
        out_specs=(VMEM, VMEM),
        scratch_shapes=[
            pltpu.SMEM((1, touch), jnp.int32),
            pltpu.VMEM((LANES, LANES), jnp.float32),
            pltpu.SemaphoreType.DMA,
        ],
    )(touched, sums)


def add_kernel(*refs):
    total = refs[0][...]
    for ref in refs[1:-1]:
        total = total + ref[...]
    refs[-1][...] = total


def add_all(parts):
    return call(
        add_kernel,
        0.2,
        1,
        out_shape=like(parts[0].shape),
        in_specs=[VMEM] * len(parts),
        out_specs=VMEM,
    )(*parts)


def update_kernel(limit, touched_hbm, *refs):
    out_hbm, new_accum_ref, fresh, listed, sems = refs[-5:]
    sums_ref, table_ref, accum_rep_ref, mean_rep_ref, accum_ref, mean_ref = refs[-12:-6]
    fetch = pltpu.make_async_copy(touched_hbm, listed, sems.at[0])
    fetch.start()
    square = refs[0][...]
    for ref in refs[1:-12]:
        square = square + ref[...]
    square = jnp.sum(jnp.sum(square, axis=1, keepdims=True), axis=0, keepdims=True)
    factor = limit / jnp.maximum(jnp.sqrt(square), limit)
    factor_sq = factor * factor
    new_accum_ref[...] = accum_ref[...] + factor_sq * mean_ref[...]
    rate = LEARN_RATE * factor
    fetch.wait()

    def step(t, _):
        accum = accum_rep_ref[t] + factor_sq * mean_rep_ref[t]
        old = table_ref[listed[0, t]]
        fresh[t] = old * (1.0 - DECAY_RATE) - (rate * sums_ref[t]) * lax.rsqrt(accum)
        pltpu.make_async_copy(fresh.at[t], out_hbm.at[listed[0, t]], sems.at[1]).start()
        return 0

    lax.fori_loop(0, fresh.shape[0], step, 0)
    pltpu.make_async_copy(fresh, fresh, sems.at[1]).wait()


def update(limit, touched, squares, sums, old, accum_rep, mean_rep, accum, mean, table):
    n = len(squares)
    return call(
        functools.partial(update_kernel, limit),
        2.5,
        8,
        out_shape=(like(table.shape, table.dtype), like(accum.shape, accum.dtype)),
        in_specs=[HBM] + [VMEM] * (n + 6) + [HBM],
        out_specs=(HBM, VMEM),
        scratch_shapes=[
            pltpu.VMEM(sums.shape, table.dtype),
            pltpu.SMEM(touched.shape, jnp.int32),
            pltpu.SemaphoreType.DMA((2,)),
        ],
        input_output_aliases={n + 7: 0},
    )(touched, *squares, sums, old, accum_rep, mean_rep, accum, mean, table)


def step(row_ids, grad_rows, touched, block_home, embed_table, row_accum):
    slots, width = grad_rows.shape[3:]
    blocks_here = embed_table.shape[0] // BLOCK
    touch = touched.shape[1]
    shards = lax.axis_size("shard")
    reps = lax.axis_size("rep")
    limit = CLIP_RMS * math.sqrt(shards * touch * BLOCK * width)
    swap = [(i, (i + 1) % reps) for i in range(reps)]
    ids, grads = row_ids[0, 0], grad_rows[0, 0]
    table = embed_table.reshape(blocks_here, BLOCK, width)
    accum = row_accum.reshape(-1, LANES)
    home = jnp.pad(block_home, (0, -block_home.shape[0] % LANES)).reshape(-1, LANES)

    data = pack(ids, grads)
    data = lax.all_to_all(data, "shard", 0, 0, tiled=True)
    table_out = keep_untouched(touched, table)
    split = shards // 2
    other_a = lax.ppermute(data[:split], "rep", swap)
    other_b = lax.ppermute(data[split:], "rep", swap)
    keys = slot_keys(touched, home, data, slots, blocks_here)
    other_keys = lax.ppermute(keys, "rep", swap)
    (sums,) = sums_of(keys, data, slots, touch)
    accum_rep = spread_accum(touched, accum)
    (sums,) = sums_of(other_keys, other_a, slots, touch, 0, sums)
    first = split * slots // LANES
    sums, square = sums_of(other_keys, other_b, slots, touch, first, sums, True)
    squares = [square]
    stride = 1
    while stride < shards:
        fan = min(4, shards // stride)
        if len(squares) > 1:
            squares = [add_all(squares)]
        squares += [
            lax.ppermute(
                squares[0], "shard", [(i, i ^ (r * stride)) for i in range(shards)]
            )
            for r in range(1, fan)
        ]
        stride *= fan
    mean_rep, mean = row_means(touched, sums, accum.shape[0])
    table_out, accum_out = update(
        limit, touched, squares, sums, table, accum_rep, mean_rep, accum, mean, table_out
    )
    return table_out.reshape(-1, width), accum_out.reshape(-1)


def solution(mesh):
    shards = mesh.shape["shard"]
    assert mesh.shape["rep"] == 2 and shards & (shards - 1) == 0
    in_specs = (
        P("rep", "shard", None, None),
        P("rep", "shard", None, None, None),
        P("shard", None),
        P(),
        P("shard", None),
        P("shard"),
    )
    out_specs = (P("shard", None), P("shard"))
    return jax.shard_map(
        step, mesh=mesh, in_specs=in_specs, out_specs=out_specs, check_vma=False
    )
```

```python
import functools
import math

import jax
import jax.numpy as jnp
from jax import lax
from jax.experimental import pallas as pl
from jax.experimental.pallas import tpu as pltpu
from jax.sharding import PartitionSpec as P

BLOCK = 256
CLIP_RMS = 0.25
LEARN_RATE = 0.1
DECAY_RATE = 0.05
LANES = 128
META = 8
PARTS = BLOCK // LANES
TILE = 2 * LANES
MIB = 1 << 20
WHOLE = 67043328


VMEM = pl.BlockSpec(memory_space=pltpu.VMEM)
HBM = pl.BlockSpec(memory_space=pltpu.HBM)


def call(kernel, us, mib, **kwargs):
    return pl.pallas_call(
        kernel,
        compiler_params=pltpu.CompilerParams(vmem_limit_bytes=int(min(mib * MIB, WHOLE))),
        cost_estimate=pl.CostEstimate(
            flops=int(us * 4e6), bytes_accessed=MIB, transcendentals=0
        ),
        **kwargs,
    )


def like(shape, dtype=jnp.float32):
    return jax.ShapeDtypeStruct(shape, dtype)


def pack_kernel(slots, blocks_here, ids_hbm, home_hbm, grads_hbm, out_ref, ids_ref, home_ref, sems):
    fetch = pltpu.make_async_copy(ids_hbm, ids_ref, sems.at[0])
    fetch_home = pltpu.make_async_copy(home_hbm, home_ref, sems.at[1])
    copy = pltpu.make_async_copy(grads_hbm, out_ref.at[:, pl.ds(0, slots), :], sems.at[2])
    fetch.start()
    fetch_home.start()
    copy.start()
    row = lax.broadcasted_iota(jnp.int32, (META, LANES), 0)
    fetch.wait()
    fetch_home.wait()
    ids = ids_ref[...]
    block = ids >> 8
    lo, hi = block & (LANES - 1), block >> 7
    home = jnp.zeros_like(ids)
    for r in range(home_ref.shape[0]):
        line = jnp.broadcast_to(home_ref[r : r + 1, :], ids.shape)
        home = jnp.where(hi == r, jnp.take_along_axis(line, lo, axis=1), home)
    owner = lax.broadcasted_iota(jnp.int32, ids.shape, 0)
    local = jnp.where(ids >= 0, home - owner * blocks_here, LANES - 1).astype(jnp.float32)
    within = (ids & (BLOCK - 1)).astype(jnp.float32)
    for group in range(ids.shape[0]):
        here = jnp.broadcast_to(local[group : group + 1, :], row.shape)
        there = jnp.broadcast_to(within[group : group + 1, :], row.shape)
        digits = jnp.where(row == 0, here, there)
        out_ref[group, slots : slots + META, :] = digits.astype(jnp.bfloat16)
    copy.wait()


def pack(ids, home, grads, blocks_here):
    groups, slots, width = grads.shape
    pad = LANES - slots
    ids = jnp.pad(ids, ((0, 0), (0, pad)), constant_values=-1) if pad else ids
    assert blocks_here < LANES
    return call(
        functools.partial(pack_kernel, slots, blocks_here),
        1.0,
        63.2,
        out_shape=like((groups, slots + META, width), grads.dtype),
        in_specs=[HBM] * 3,
        out_specs=VMEM,
        scratch_shapes=[
            pltpu.VMEM((groups, LANES), jnp.int32),
            pltpu.VMEM(home.shape, jnp.int32),
            pltpu.SemaphoreType.DMA((3,)),
        ],
    )(ids, home, grads)


def keep_kernel(touched_hbm, table_hbm, out_hbm, slot_ref, listed, bounce, other, sems):
    blocks, touch = table_hbm.shape[0], touched_hbm.shape[1]
    fetch = pltpu.make_async_copy(touched_hbm, listed, sems.at[0])
    fetch.start()

    def clear(b, _):
        other[b] = 0
        return 0

    lax.fori_loop(0, blocks, clear, 0)
    fetch.wait()

    lane = lax.broadcasted_iota(jnp.int32, slot_ref.shape, 1)

    def mark(t, slot):
        b = listed[0, t]
        other[b] = 1
        return jnp.where(lane == b, t, slot)

    slot_ref[...] = lax.fori_loop(0, touch, mark, jnp.full(slot_ref.shape, -1, jnp.int32))

    def pull(b, count):
        free = other[b] == 0

        @pl.when(free)
        def _():
            pltpu.make_async_copy(table_hbm.at[b], bounce.at[count], sems.at[1]).start()
            other[blocks + count] = b

        return count + free.astype(jnp.int32)

    lax.fori_loop(0, blocks, pull, 0)
    pltpu.make_async_copy(bounce, bounce, sems.at[1]).wait()

    def put(j, _):
        b = other[blocks + j]
        pltpu.make_async_copy(bounce.at[j], out_hbm.at[b], sems.at[2]).start()
        return 0

    lax.fori_loop(0, blocks - touch, put, 0)
    pltpu.make_async_copy(bounce, bounce, sems.at[2]).wait()


def keep_untouched(touched, table):
    blocks, _, width = table.shape
    touch = touched.shape[1]
    return call(
        keep_kernel,
        4.0,
        60,
        out_shape=(like(table.shape, table.dtype), like((8, LANES), jnp.int32)),
        in_specs=[HBM, HBM],
        out_specs=(HBM, VMEM),
        scratch_shapes=[
            pltpu.SMEM((1, touch), jnp.int32),
            pltpu.VMEM((blocks - touch, BLOCK, width), table.dtype),
            pltpu.SMEM((2 * blocks,), jnp.int32),
            pltpu.SemaphoreType.DMA((3,)),
        ],
    )(touched, table)


def slot_keys(slot_ref, data_ref, slots):
    groups = data_ref.shape[0]
    per = LANES // slots
    lane = lax.broadcasted_iota(jnp.int32, (1, LANES), 1)
    meta = data_ref[:, slots : slots + META, :].astype(jnp.float32)
    local, within = (meta[:, i, :].astype(jnp.int32) for i in range(2))
    table = jnp.broadcast_to(slot_ref[0:1, :], local.shape)
    slot = jnp.take_along_axis(table, local, axis=1)
    keys = jnp.where(slot >= 0, slot * BLOCK + within, -1)
    lines = []
    for g in range(groups // per):
        line = keys[g * per : g * per + 1, :]
        for j in range(1, per):
            key = pltpu.roll(keys[g * per + j : g * per + j + 1, :], j * slots, 1)
            line = jnp.where((lane >= j * slots) & (lane < (j + 1) * slots), key, line)
        lines.append(line)
    return lines


def add_rows(slots, fresh, squared, slot_ref, data_ref, *refs):
    sums_ref, weights = refs[0 if fresh else 1], refs[-1]
    touch, _, width = sums_ref.shape
    per = TILE // slots
    tiles = data_ref.shape[0] // per
    many = next(m for m in (4, 2, 1) if touch % m == 0)
    lines = slot_keys(slot_ref, data_ref, slots)
    key_rows = []
    for k in range(tiles):
        pair = lines[2 * k : 2 * k + 2]
        upper = [((key >> 7) & 1).astype(jnp.float32) for key in pair]
        upper = [jnp.broadcast_to(u, (LANES, LANES)).T for u in upper]
        upper = jnp.concatenate(upper, axis=0).astype(jnp.bfloat16)
        rows = data_ref[k * per : (k + 1) * per, 0:slots, :].reshape(TILE, width)
        high = rows * upper
        weights[k, :, width : 2 * width] = high
        weights[k, :, 0:width] = rows - high
        flat = [jnp.where(key >= 0, (key >> 8) * LANES + (key & (LANES - 1)), -1) for key in pair]
        key_rows.append(jnp.concatenate(flat, axis=1))
    row = lax.broadcasted_iota(jnp.int32, (many * LANES, TILE), 0)

    def step(u, carry):
        total = None
        for k in range(tiles):
            match = row == jnp.broadcast_to(key_rows[k] - u * (many * LANES), row.shape)
            onehot = jnp.where(match, 1.0, 0.0).astype(jnp.bfloat16)
            part = jnp.dot(onehot, weights[k], preferred_element_type=jnp.float32)
            total = part if total is None else total + part
        for i in range(many):
            t = u * many + i
            for p in range(PARTS):
                piece = total[i * LANES : (i + 1) * LANES, p * width : (p + 1) * width]
                at = pl.ds(p * LANES, LANES)
                piece = piece if fresh else piece + sums_ref[t, at, :]
                sums_ref[t, at, :] = piece
                if squared:
                    carry = carry + jnp.sum((piece * piece).reshape(-1, 8, width), axis=0)
        return carry

    carry = jnp.zeros((8, width), jnp.float32) if squared else 0
    carry = lax.fori_loop(0, touch // many, step, carry)
    if squared:
        refs[-2][...] = carry


def sums_of(slot, data, slots, touch, sums=None, squared=False):
    width = data.shape[-1]
    fresh = sums is None
    return call(
        functools.partial(add_rows, slots, fresh, squared),
        data.shape[0] * slots / 512,
        10,
        out_shape=(like((touch, BLOCK, width)), like((8, width)))[: 1 + squared],
        in_specs=[VMEM] * (2 if fresh else 3),
        out_specs=(VMEM, VMEM)[: 1 + squared],
        scratch_shapes=[
            pltpu.VMEM((data.shape[0] * slots // TILE, TILE, 2 * width), data.dtype)
        ],
        input_output_aliases={} if fresh else {2: 0},
    )(slot, data, *([] if fresh else [sums]))


def spread_kernel(touched_hbm, accum_hbm, rep_ref, listed, accum, sems):
    a = pltpu.make_async_copy(touched_hbm, listed, sems.at[0])
    b = pltpu.make_async_copy(accum_hbm, accum, sems.at[1])
    a.start()
    b.start()
    a.wait()
    b.wait()

    def step(t, _):
        for part in range(PARTS):
            row = accum[pl.ds(listed[0, t] * PARTS + part, 1), :]
            rep_ref[t, part * LANES : (part + 1) * LANES, :] = jnp.broadcast_to(
                row, (LANES, LANES)
            ).T
        return 0

    lax.fori_loop(0, rep_ref.shape[0], step, 0)


def spread_accum(touched, accum):
    touch = touched.shape[1]
    return call(
        spread_kernel,
        2.0,
        8,
        out_shape=like((touch, BLOCK, LANES)),
        in_specs=[HBM, HBM],
        out_specs=VMEM,
        scratch_shapes=[
            pltpu.SMEM((1, touch), jnp.int32),
            pltpu.VMEM(accum.shape, accum.dtype),
            pltpu.SemaphoreType.DMA((2,)),
        ],
    )(touched, accum)


def means_kernel(touched_hbm, sums_ref, rep_ref, flat_ref, listed, turned, sem):
    touch, _, width = sums_ref.shape
    fetch = pltpu.make_async_copy(touched_hbm, listed, sem)
    fetch.start()
    flat_ref[...] = jnp.zeros_like(flat_ref)
    lane = lax.broadcasted_iota(jnp.int32, (LANES, LANES), 1)

    def step(t, gathered):
        total = sums_ref[t]
        square = total * total * (1.0 / width)
        wide = jnp.broadcast_to(jnp.sum(square, axis=1, keepdims=True), (BLOCK, LANES))
        rep_ref[t] = wide
        for part in range(PARTS):
            piece = wide[part * LANES : (part + 1) * LANES, :]
            gathered = jnp.where(lane == t * PARTS + part, piece, gathered)
        return gathered

    gathered = lax.fori_loop(0, touch, step, jnp.zeros((LANES, LANES), jnp.float32))
    turned[...] = gathered.T
    fetch.wait()
    for t in range(touch):
        for part in range(PARTS):
            j = t * PARTS + part
            flat_ref[pl.ds(listed[0, t] * PARTS + part, 1), :] = turned[j : j + 1, :]


def row_means(touched, sums, accum_rows):
    touch = touched.shape[1]
    assert touch * PARTS <= LANES
    return call(
        means_kernel,
        2.0,
        8,
        out_shape=(like((touch, BLOCK, LANES)), like((accum_rows, LANES))),
        in_specs=[HBM, VMEM],
        out_specs=(VMEM, VMEM),
        scratch_shapes=[
            pltpu.SMEM((1, touch), jnp.int32),
            pltpu.VMEM((LANES, LANES), jnp.float32),
            pltpu.SemaphoreType.DMA,
        ],
    )(touched, sums)


def add_kernel(*refs):
    total = refs[0][...]
    for ref in refs[1:-1]:
        total = total + ref[...]
    refs[-1][...] = total


def add_all(parts):
    return call(
        add_kernel,
        0.2,
        1,
        out_shape=like(parts[0].shape),
        in_specs=[VMEM] * len(parts),
        out_specs=VMEM,
    )(*parts)


def update_kernel(limit, touched_hbm, *refs):
    out_hbm, new_accum_hbm, fresh, new_accum, listed, sems = refs[-6:]
    sums_ref, table_ref, accum_rep_ref, mean_rep_ref, accum_ref, mean_ref = refs[-13:-7]
    fetch = pltpu.make_async_copy(touched_hbm, listed, sems.at[0])
    fetch.start()
    square = refs[0][...]
    for ref in refs[1:-13]:
        square = square + ref[...]
    square = jnp.sum(jnp.sum(square, axis=1, keepdims=True), axis=0, keepdims=True)
    factor = limit / jnp.maximum(jnp.sqrt(square), limit)
    factor_sq = factor * factor
    new_accum[...] = accum_ref[...] + factor_sq * mean_ref[...]
    put = pltpu.make_async_copy(new_accum, new_accum_hbm, sems.at[2])
    put.start()
    rate = LEARN_RATE * factor
    fetch.wait()

    def step(t, _):
        accum = accum_rep_ref[t] + factor_sq * mean_rep_ref[t]
        old = table_ref[listed[0, t]]
        fresh[t] = old * (1.0 - DECAY_RATE) - (rate * sums_ref[t]) * lax.rsqrt(accum)
        pltpu.make_async_copy(fresh.at[t], out_hbm.at[listed[0, t]], sems.at[1]).start()
        return 0

    lax.fori_loop(0, fresh.shape[0], step, 0)
    put.wait()
    pltpu.make_async_copy(fresh, fresh, sems.at[1]).wait()


def update(limit, touched, squares, sums, old, accum_rep, mean_rep, accum, mean, table):
    n = len(squares)
    return call(
        functools.partial(update_kernel, limit),
        2.5,
        8,
        out_shape=(like(table.shape, table.dtype), like(accum.shape, accum.dtype)),
        in_specs=[HBM] + [VMEM] * (n + 6) + [HBM],
        out_specs=(HBM, HBM),
        scratch_shapes=[
            pltpu.VMEM(sums.shape, table.dtype),
            pltpu.VMEM(accum.shape, accum.dtype),
            pltpu.SMEM(touched.shape, jnp.int32),
            pltpu.SemaphoreType.DMA((3,)),
        ],
        input_output_aliases={n + 7: 0},
    )(touched, *squares, sums, old, accum_rep, mean_rep, accum, mean, table)


def step(row_ids, grad_rows, touched, block_home, embed_table, row_accum):
    slots, width = grad_rows.shape[3:]
    blocks_here = embed_table.shape[0] // BLOCK
    touch = touched.shape[1]
    shards = lax.axis_size("shard")
    reps = lax.axis_size("rep")
    limit = CLIP_RMS * math.sqrt(shards * touch * BLOCK * width)
    swap = [(i, (i + 1) % reps) for i in range(reps)]
    ids, grads = row_ids[0, 0], grad_rows[0, 0]
    table = embed_table.reshape(blocks_here, BLOCK, width)
    accum = row_accum.reshape(-1, LANES)
    home = jnp.pad(block_home, (0, -block_home.shape[0] % LANES)).reshape(-1, LANES)

    data = pack(ids, home, grads, blocks_here)
    data = lax.all_to_all(data, "shard", 0, 0, tiled=True)
    table_out, slot = keep_untouched(touched, table)
    split = shards // 2
    other_a = lax.ppermute(data[:split], "rep", swap)
    other_b = lax.ppermute(data[split:], "rep", swap)
    (sums,) = sums_of(slot, data, slots, touch)
    accum_rep = spread_accum(touched, accum)
    (sums,) = sums_of(slot, other_a, slots, touch, sums)
    sums, square = sums_of(slot, other_b, slots, touch, sums, True)
    squares = [square]
    stride = 1
    while stride < shards:
        fan = min(4, shards // stride)
        if len(squares) > 1:
            squares = [add_all(squares)]
        squares += [
            lax.ppermute(
                squares[0], "shard", [(i, i ^ (r * stride)) for i in range(shards)]
            )
            for r in range(1, fan)
        ]
        stride = stride * fan
    mean_rep, mean = row_means(touched, sums, accum.shape[0])
    table_out, accum_out = update(
        limit, touched, squares, sums, table, accum_rep, mean_rep, accum, mean, table_out
    )
    return table_out.reshape(-1, width), accum_out.reshape(-1)


def solution(mesh):
    shards = mesh.shape["shard"]
    assert mesh.shape["rep"] == 2 and shards & (shards - 1) == 0
    in_specs = (
        P("rep", "shard", None, None),
        P("rep", "shard", None, None, None),
        P("shard", None),
        P(),
        P("shard", None),
        P("shard"),
    )
    out_specs = (P("shard", None), P("shard"))
    return jax.shard_map(
        step, mesh=mesh, in_specs=in_specs, out_specs=out_specs, check_vma=False
    )
```

```python
import functools
import math

import jax
import jax.numpy as jnp
from jax import lax
from jax.experimental import pallas as pl
from jax.experimental.pallas import tpu as pltpu
from jax.sharding import PartitionSpec as P

BLOCK = 256
CLIP_RMS = 0.25
LEARN_RATE = 0.1
DECAY_RATE = 0.05
LANES = 128
META = 8
PARTS = BLOCK // LANES
TILE = 2 * LANES
MIB = 1 << 20
WHOLE = 67043328


VMEM = pl.BlockSpec(memory_space=pltpu.VMEM)
HBM = pl.BlockSpec(memory_space=pltpu.HBM)

EARLY = 4


def call(kernel, us, mib, **kwargs):
    return pl.pallas_call(
        kernel,
        compiler_params=pltpu.CompilerParams(vmem_limit_bytes=int(min(mib * MIB, WHOLE))),
        cost_estimate=pl.CostEstimate(
            flops=int(us * 4e6), bytes_accessed=MIB, transcendentals=0
        ),
        **kwargs,
    )


def like(shape, dtype=jnp.float32):
    return jax.ShapeDtypeStruct(shape, dtype)


def pack_kernel(slots, blocks_here, ids_hbm, home_hbm, grads_hbm, out_ref, *rest):
    early, (ids_ref, home_ref, digits_ref, sems) = rest[:-4], rest[-4:]
    fetch = pltpu.make_async_copy(ids_hbm, ids_ref, sems.at[0])
    fetch_home = pltpu.make_async_copy(home_hbm, home_ref, sems.at[1])
    copy = pltpu.make_async_copy(grads_hbm, out_ref.at[:, pl.ds(0, slots), :], sems.at[2])
    fetch.start()
    fetch_home.start()
    copy.start()
    me = lax.axis_index("shard")
    copies = [
        pltpu.make_async_copy(
            grads_hbm.at[me ^ r], early[r].at[0, pl.ds(0, slots), :], sems.at[3 + r]
        )
        for r in range(len(early))
    ]
    for each in copies:
        each.start()
    row = lax.broadcasted_iota(jnp.int32, (META, LANES), 0)
    fetch.wait()
    fetch_home.wait()
    ids = ids_ref[...]
    block = ids >> 8
    lo, hi = block & (LANES - 1), block >> 7
    home = jnp.zeros_like(ids)
    for r in range(home_ref.shape[0]):
        line = jnp.broadcast_to(home_ref[r : r + 1, :], ids.shape)
        home = jnp.where(hi == r, jnp.take_along_axis(line, lo, axis=1), home)
    owner = lax.broadcasted_iota(jnp.int32, ids.shape, 0)
    local = jnp.where(ids >= 0, home - owner * blocks_here, LANES - 1).astype(jnp.float32)
    within = (ids & (BLOCK - 1)).astype(jnp.float32)
    for group in range(ids.shape[0]):
        here = jnp.broadcast_to(local[group : group + 1, :], row.shape)
        there = jnp.broadcast_to(within[group : group + 1, :], row.shape)
        digits = jnp.where(row == 0, here, there)
        out_ref[group, slots : slots + META, :] = digits.astype(jnp.bfloat16)
        digits_ref[group] = digits
    for r, ref in enumerate(early):
        ref[0, slots : slots + META, :] = digits_ref[me ^ r].astype(jnp.bfloat16)
    for each in copies:
        each.wait()
    copy.wait()


def pack(ids, home, grads, blocks_here, early):
    groups, slots, width = grads.shape
    pad = LANES - slots
    ids = jnp.pad(ids, ((0, 0), (0, pad)), constant_values=-1) if pad else ids
    assert blocks_here < LANES
    slab = (slots + META, width)
    return call(
        functools.partial(pack_kernel, slots, blocks_here),
        1.0,
        62.9,
        out_shape=(like((groups, *slab), grads.dtype),)
        + (like((1, *slab), grads.dtype),) * early,
        in_specs=[HBM] * 3,
        out_specs=(VMEM,) * (1 + early),
        scratch_shapes=[
            pltpu.VMEM((groups, LANES), jnp.int32),
            pltpu.VMEM(home.shape, jnp.int32),
            pltpu.VMEM((groups, META, LANES), jnp.float32),
            pltpu.SemaphoreType.DMA((3 + early,)),
        ],
    )(ids, home, grads)


def pick_kernel(group, data_ref, first_ref, second_ref):
    groups = data_ref.shape[0] // group
    mine = lax.axis_index("shard") // group
    first = first_ref.shape[0]
    for j in range(group, groups * group):
        where = lax.rem(mine + j // group, groups) * group + j % group
        at = j - group
        if at < first:
            first_ref[at] = data_ref[where]
        else:
            second_ref[at - first] = data_ref[where]


def pick_far(data, group):
    groups, *slab = data.shape
    last = (groups - group) // 3
    return call(
        functools.partial(pick_kernel, group),
        0.5,
        4,
        out_shape=(
            like((groups - group - last, *slab), data.dtype),
            like((last, *slab), data.dtype),
        ),
        in_specs=[VMEM],
        out_specs=(VMEM, VMEM),
    )(data)


def keep_kernel(touched_hbm, table_hbm, out_hbm, slot_ref, listed, bounce, other, sems):
    blocks, touch = table_hbm.shape[0], touched_hbm.shape[1]
    fetch = pltpu.make_async_copy(touched_hbm, listed, sems.at[0])
    fetch.start()

    def clear(b, _):
        other[b] = 0
        return 0

    lax.fori_loop(0, blocks, clear, 0)
    fetch.wait()

    lane = lax.broadcasted_iota(jnp.int32, slot_ref.shape, 1)

    def mark(t, slot):
        b = listed[0, t]
        other[b] = 1
        return jnp.where(lane == b, t, slot)

    slot_ref[...] = lax.fori_loop(0, touch, mark, jnp.full(slot_ref.shape, -1, jnp.int32))

    def pull(b, count):
        free = other[b] == 0

        @pl.when(free)
        def _():
            pltpu.make_async_copy(table_hbm.at[b], bounce.at[count], sems.at[1]).start()
            other[blocks + count] = b

        return count + free.astype(jnp.int32)

    lax.fori_loop(0, blocks, pull, 0)
    pltpu.make_async_copy(bounce, bounce, sems.at[1]).wait()

    def put(j, _):
        b = other[blocks + j]
        pltpu.make_async_copy(bounce.at[j], out_hbm.at[b], sems.at[2]).start()
        return 0

    lax.fori_loop(0, blocks - touch, put, 0)
    pltpu.make_async_copy(bounce, bounce, sems.at[2]).wait()


def keep_untouched(touched, table):
    blocks, _, width = table.shape
    touch = touched.shape[1]
    return call(
        keep_kernel,
        4.0,
        60,
        out_shape=(like(table.shape, table.dtype), like((8, LANES), jnp.int32)),
        in_specs=[HBM, HBM],
        out_specs=(HBM, VMEM),
        scratch_shapes=[
            pltpu.SMEM((1, touch), jnp.int32),
            pltpu.VMEM((blocks - touch, BLOCK, width), table.dtype),
            pltpu.SMEM((2 * blocks,), jnp.int32),
            pltpu.SemaphoreType.DMA((3,)),
        ],
    )(touched, table)


def slot_keys(slot_ref, slabs, slots):
    per = LANES // slots
    lane = lax.broadcasted_iota(jnp.int32, (1, LANES), 1)
    table = jnp.broadcast_to(slot_ref[0:1, :], (META, LANES))
    keys = []
    for ref, i in slabs:
        meta = ref[i, slots : slots + META, :].astype(jnp.float32).astype(jnp.int32)
        local = jnp.broadcast_to(meta[0:1, :], (META, LANES))
        slot = jnp.take_along_axis(table, local, axis=1)[0:1, :]
        keys.append(jnp.where(slot >= 0, slot * BLOCK + meta[1:2, :], -1))
    lines = []
    for g in range(len(slabs) // per):
        line = keys[g * per]
        for j in range(1, per):
            key = pltpu.roll(keys[g * per + j], j * slots, 1)
            line = jnp.where((lane >= j * slots) & (lane < (j + 1) * slots), key, line)
        lines.append(line)
    return lines


def add_rows(slots, count, fresh, last, slot_ref, *refs):
    data, refs = refs[:count], refs[count:]
    sums_ref, weights = refs[0 if fresh else 1], refs[-1]
    touch, _, width = sums_ref.shape
    per = TILE // slots
    slabs = [(ref, i) for ref in data for i in range(ref.shape[0])]
    tiles = len(slabs) // per
    many = next(m for m in (4, 2, 1) if touch % m == 0)
    lines = slot_keys(slot_ref, slabs, slots)
    key_rows = []
    for k in range(tiles):
        pair = lines[2 * k : 2 * k + 2]
        upper = [((key >> 7) & 1).astype(jnp.float32) for key in pair]
        upper = [jnp.broadcast_to(u, (LANES, LANES)).T for u in upper]
        upper = jnp.concatenate(upper, axis=0).astype(jnp.bfloat16)
        rows = [ref[i, 0:slots, :] for ref, i in slabs[k * per : (k + 1) * per]]
        rows = jnp.concatenate(rows, axis=0)
        high = rows * upper
        weights[k, :, width : 2 * width] = high
        weights[k, :, 0:width] = rows - high
        flat = [jnp.where(key >= 0, (key >> 8) * LANES + (key & (LANES - 1)), -1) for key in pair]
        key_rows.append(jnp.concatenate(flat, axis=1))
    row = lax.broadcasted_iota(jnp.int32, (many * LANES, TILE), 0)
    lane = lax.broadcasted_iota(jnp.int32, (LANES, LANES), 1)
    if last:
        mean_rep_ref, gathered_ref, square_ref = refs[2:5]
        gathered_ref[...] = jnp.zeros_like(gathered_ref)

    def step(u, carry):
        total = None
        for k in range(tiles):
            match = row == jnp.broadcast_to(key_rows[k] - u * (many * LANES), row.shape)
            onehot = jnp.where(match, 1.0, 0.0).astype(jnp.bfloat16)
            part = jnp.dot(onehot, weights[k], preferred_element_type=jnp.float32)
            total = part if total is None else total + part
        for i in range(many):
            t = u * many + i
            for p in range(PARTS):
                piece = total[i * LANES : (i + 1) * LANES, p * width : (p + 1) * width]
                at = pl.ds(p * LANES, LANES)
                piece = piece if fresh else piece + sums_ref[t, at, :]
                sums_ref[t, at, :] = piece
                if last:
                    mean = jnp.sum(piece * piece, axis=1, keepdims=True) * (1.0 / width)
                    mean = jnp.broadcast_to(mean, (LANES, LANES))
                    mean_rep_ref[t, at, :] = mean
                    gathered_ref[...] = jnp.where(
                        lane == t * PARTS + p, mean, gathered_ref[...]
                    )
        return carry

    lax.fori_loop(0, touch // many, step, 0)
    if last:
        square = jnp.sum(gathered_ref[...].reshape(-1, 8, LANES), axis=0) * width
        for i in range(square_ref.shape[0]):
            square_ref[i] = square


def sums_of(slot, data, slots, touch, sums=None, shards=0):
    width = data[0].shape[-1]
    count = len(data)
    slabs = sum(each.shape[0] for each in data)
    fresh, last = sums is None, shards > 0
    assert slabs * slots % TILE == 0 and touch * PARTS <= LANES
    outs = (like((touch, BLOCK, width)),)
    if last:
        outs += (like((touch, BLOCK, LANES)), like((LANES, LANES)), like((shards, 8, LANES)))
    return call(
        functools.partial(add_rows, slots, count, fresh, last),
        slabs * slots / 512,
        10,
        out_shape=outs,
        in_specs=[VMEM] * (1 + count + (not fresh)),
        out_specs=(VMEM,) * len(outs),
        scratch_shapes=[pltpu.VMEM((slabs * slots // TILE, TILE, 2 * width), data[0].dtype)],
        input_output_aliases={} if fresh else {1 + count: 0},
    )(slot, *data, *([] if fresh else [sums]))


def spread_kernel(touched_hbm, accum_hbm, rep_ref, listed, accum, sems):
    a = pltpu.make_async_copy(touched_hbm, listed, sems.at[0])
    b = pltpu.make_async_copy(accum_hbm, accum, sems.at[1])
    a.start()
    b.start()
    a.wait()
    b.wait()

    def step(t, _):
        for part in range(PARTS):
            row = accum[pl.ds(listed[0, t] * PARTS + part, 1), :]
            rep_ref[t, part * LANES : (part + 1) * LANES, :] = jnp.broadcast_to(
                row, (LANES, LANES)
            ).T
        return 0

    lax.fori_loop(0, rep_ref.shape[0], step, 0)


def spread_accum(touched, accum):
    touch = touched.shape[1]
    return call(
        spread_kernel,
        2.0,
        8,
        out_shape=like((touch, BLOCK, LANES)),
        in_specs=[HBM, HBM],
        out_specs=VMEM,
        scratch_shapes=[
            pltpu.SMEM((1, touch), jnp.int32),
            pltpu.VMEM(accum.shape, accum.dtype),
            pltpu.SemaphoreType.DMA((2,)),
        ],
    )(touched, accum)


def update_kernel(
    limit, touched_hbm, square_ref, sums_ref, table_ref, accum_rep_ref, mean_rep_ref,
    gathered_ref, accum_hbm, table_in, out_hbm, new_accum_hbm,
    fresh, turned, accum, listed, sems,
):
    fetch = pltpu.make_async_copy(touched_hbm, listed, sems.at[0])
    fetch_accum = pltpu.make_async_copy(accum_hbm, accum, sems.at[1])
    fetch.start()
    fetch_accum.start()
    touch = fresh.shape[0]
    square = jnp.sum(square_ref[...], axis=0)
    square = jnp.sum(jnp.sum(square, axis=1, keepdims=True), axis=0, keepdims=True)
    turned[...] = gathered_ref[...].T
    factor = limit / jnp.maximum(jnp.sqrt(square), limit)
    factor_sq = factor * factor
    rate = LEARN_RATE * factor
    fetch.wait()

    def step(t, _):
        b = listed[0, t]
        root = lax.rsqrt(accum_rep_ref[t] + factor_sq * mean_rep_ref[t])
        fresh[t] = table_ref[b] * (1.0 - DECAY_RATE) - (rate * sums_ref[t]) * root
        pltpu.make_async_copy(fresh.at[t], out_hbm.at[b], sems.at[2]).start()
        return 0

    fetch_accum.wait()
    for t in range(touch):
        for part in range(PARTS):
            at = pl.ds(listed[0, t] * PARTS + part, 1)
            j = t * PARTS + part
            accum[at, :] = accum[at, :] + factor_sq * turned[j : j + 1, :]
    put = pltpu.make_async_copy(accum, new_accum_hbm, sems.at[3])
    put.start()
    lax.fori_loop(0, touch, step, 0)
    put.wait()
    pltpu.make_async_copy(fresh, fresh, sems.at[2]).wait()


def update(limit, touched, square, sums, table, accum_rep, mean_rep, gathered, accum, table_out):
    return call(
        functools.partial(update_kernel, limit),
        2.5,
        8,
        out_shape=(like(table.shape, table.dtype), like(accum.shape, accum.dtype)),
        in_specs=[HBM] + [VMEM] * 6 + [HBM] * 2,
        out_specs=(HBM, HBM),
        scratch_shapes=[
            pltpu.VMEM(sums.shape, table.dtype),
            pltpu.VMEM((LANES, LANES), jnp.float32),
            pltpu.VMEM(accum.shape, accum.dtype),
            pltpu.SMEM(touched.shape, jnp.int32),
            pltpu.SemaphoreType.DMA((4,)),
        ],
        input_output_aliases={8: 0},
    )(touched, square, sums, table, accum_rep, mean_rep, gathered, accum, table_out)


def exchange(x):
    return lax.all_to_all(x, "shard", 0, 0, tiled=True)


def step(row_ids, grad_rows, touched, block_home, embed_table, row_accum):
    slots, width = grad_rows.shape[3:]
    blocks_here = embed_table.shape[0] // BLOCK
    touch = touched.shape[1]
    shards = lax.axis_size("shard")
    reps = lax.axis_size("rep")
    limit = CLIP_RMS * math.sqrt(shards * touch * BLOCK * width)
    ids, grads = row_ids[0, 0], grad_rows[0, 0]
    table = embed_table.reshape(blocks_here, BLOCK, width)
    accum = row_accum.reshape(-1, LANES)
    home = jnp.pad(block_home, (0, -block_home.shape[0] % LANES)).reshape(-1, LANES)
    direct = EARLY if shards > EARLY and EARLY * slots >= TILE else 0

    def swap(x, r=0):
        pairs = [
            (rep * shards + i, (rep + 1) % reps * shards + (i ^ r))
            for rep in range(reps)
            for i in range(shards)
        ]
        return lax.ppermute(x, ("rep", "shard"), pairs)

    data, *early = pack(ids, home, grads, blocks_here, direct)
    data = exchange(data)
    early = [swap(each, r) for r, each in enumerate(early)]
    table_out, slot = keep_untouched(touched, table)
    if direct:
        far_a, far_b = pick_far(data, direct)
    else:
        far_a, far_b = data[: shards // 2], data[shards // 2 :]
    far_a = swap(far_a)
    far_b = swap(far_b)
    (sums,) = sums_of(slot, [data], slots, touch)
    if direct:
        (sums,) = sums_of(slot, early, slots, touch, sums)
    accum_rep = spread_accum(touched, accum)
    (sums,) = sums_of(slot, [far_a], slots, touch, sums)
    sums, mean_rep, gathered, square = sums_of(slot, [far_b], slots, touch, sums, shards)
    square = exchange(square)
    table_out, accum_out = update(
        limit, touched, square, sums, table, accum_rep, mean_rep, gathered, accum, table_out
    )
    return table_out.reshape(-1, width), accum_out.reshape(-1)


def solution(mesh):
    shards = mesh.shape["shard"]
    assert mesh.shape["rep"] == 2 and shards & (shards - 1) == 0
    in_specs = (
        P("rep", "shard", None, None),
        P("rep", "shard", None, None, None),
        P("shard", None),
        P(),
        P("shard", None),
        P("shard"),
    )
    out_specs = (P("shard", None), P("shard"))
    return jax.shard_map(step, mesh=mesh, in_specs=in_specs, out_specs=out_specs, check_vma=False)
```

```python
import functools
import math

import jax
import jax.numpy as jnp
from jax import lax
from jax.experimental import pallas as pl
from jax.experimental.pallas import tpu as pltpu
from jax.sharding import PartitionSpec as P

BLOCK = 256
CLIP_RMS = 0.25
LEARN_RATE = 0.1
DECAY_RATE = 0.05
LANES = 128
META = 8
PARTS = BLOCK // LANES
TILE = 2 * LANES
MIB = 1 << 20
WHOLE = 67043328


VMEM = pl.BlockSpec(memory_space=pltpu.VMEM)
HBM = pl.BlockSpec(memory_space=pltpu.HBM)

EARLY = 4
CHUNKS = 4


def call(kernel, us, mib, **kwargs):
    return pl.pallas_call(
        kernel,
        compiler_params=pltpu.CompilerParams(vmem_limit_bytes=int(min(mib * MIB, WHOLE))),
        cost_estimate=pl.CostEstimate(
            flops=int(us * 4e6), bytes_accessed=MIB, transcendentals=0
        ),
        **kwargs,
    )


def like(shape, dtype=jnp.float32):
    return jax.ShapeDtypeStruct(shape, dtype)


def pack_kernel(slots, blocks_here, ids_hbm, home_hbm, grads_hbm, out_hbm, *rest):
    early, (ids_ref, home_ref, buffer, sems, load_sems) = rest[:-5], rest[-5:]
    groups = ids_ref.shape[0]
    fetch = pltpu.make_async_copy(ids_hbm, ids_ref, sems.at[0])
    fetch_home = pltpu.make_async_copy(home_hbm, home_ref, sems.at[1])
    fetch.start()
    fetch_home.start()
    chunk = groups // CHUNKS
    loads = []
    for c in range(CHUNKS):
        at = pl.ds(c * chunk, chunk)
        loads.append(
            pltpu.make_async_copy(
                grads_hbm.at[at], buffer.at[at, pl.ds(0, slots), :], load_sems.at[c]
            )
        )
        loads[c].start()
    row = lax.broadcasted_iota(jnp.int32, (META, LANES), 0)
    fetch.wait()
    fetch_home.wait()
    ids = ids_ref[...]
    block = ids >> 8
    lo, hi = block & (LANES - 1), block >> 7
    home = jnp.zeros_like(ids)
    for r in range(home_ref.shape[0]):
        line = jnp.broadcast_to(home_ref[r : r + 1, :], ids.shape)
        home = jnp.where(hi == r, jnp.take_along_axis(line, lo, axis=1), home)
    owner = lax.broadcasted_iota(jnp.int32, ids.shape, 0)
    local = jnp.where(ids >= 0, home - owner * blocks_here, LANES - 1).astype(jnp.float32)
    within = (ids & (BLOCK - 1)).astype(jnp.float32)
    for group in range(groups):
        here = jnp.broadcast_to(local[group : group + 1, :], row.shape)
        there = jnp.broadcast_to(within[group : group + 1, :], row.shape)
        digits = jnp.where(row == 0, here, there)
        buffer[group, slots : slots + META, :] = digits.astype(jnp.bfloat16)
    stores = []
    for c in range(CHUNKS):
        loads[c].wait()
        at = pl.ds(c * chunk, chunk)
        stores.append(pltpu.make_async_copy(buffer.at[at], out_hbm.at[at], load_sems.at[c]))
        stores[c].start()
    me = lax.axis_index("shard")
    for r, ref in enumerate(early):
        stores.append(pltpu.make_async_copy(buffer.at[me ^ r], ref.at[0], sems.at[2 + r]))
        stores[-1].start()
    for each in stores:
        each.wait()


def pack(ids, home, grads, blocks_here, early):
    groups, slots, width = grads.shape
    pad = LANES - slots
    ids = jnp.pad(ids, ((0, 0), (0, pad)), constant_values=-1) if pad else ids
    assert blocks_here < LANES and groups % CHUNKS == 0
    slab = (slots + META, width)
    return call(
        functools.partial(pack_kernel, slots, blocks_here),
        1.0,
        64,
        out_shape=(like((groups, *slab), grads.dtype),)
        + (like((1, *slab), grads.dtype),) * early,
        in_specs=[HBM] * 3,
        out_specs=(HBM,) * (1 + early),
        scratch_shapes=[
            pltpu.VMEM((groups, LANES), jnp.int32),
            pltpu.VMEM(home.shape, jnp.int32),
            pltpu.VMEM((groups, *slab), grads.dtype),
            pltpu.SemaphoreType.DMA((2 + early,)),
            pltpu.SemaphoreType.DMA((CHUNKS,)),
        ],
    )(ids, home, grads)


def pick_kernel(group, data_ref, first_ref, second_ref):
    groups = data_ref.shape[0] // group
    mine = lax.axis_index("shard") // group
    first = first_ref.shape[0]
    for j in range(group, groups * group):
        where = lax.rem(mine + j // group, groups) * group + j % group
        at = j - group
        if at < first:
            first_ref[at] = data_ref[where]
        else:
            second_ref[at - first] = data_ref[where]


def pick_far(data, group):
    groups, *slab = data.shape
    last = (groups - group) // 3
    return call(
        functools.partial(pick_kernel, group),
        0.5,
        4,
        out_shape=(
            like((groups - group - last, *slab), data.dtype),
            like((last, *slab), data.dtype),
        ),
        in_specs=[VMEM],
        out_specs=(VMEM, VMEM),
    )(data)


def keep_kernel(touched_hbm, table_hbm, out_hbm, listed, bounce, other, sems):
    blocks, touch = table_hbm.shape[0], touched_hbm.shape[1]
    fetch = pltpu.make_async_copy(touched_hbm, listed, sems.at[0])
    fetch.start()

    def clear(b, _):
        other[b] = 0
        return 0

    lax.fori_loop(0, blocks, clear, 0)
    fetch.wait()

    def mark(t, _):
        other[listed[0, t]] = 1
        return 0

    lax.fori_loop(0, touch, mark, 0)

    def pull(b, count):
        free = other[b] == 0

        @pl.when(free)
        def _():
            pltpu.make_async_copy(table_hbm.at[b], bounce.at[count], sems.at[1]).start()
            other[blocks + count] = b

        return count + free.astype(jnp.int32)

    lax.fori_loop(0, blocks, pull, 0)
    pltpu.make_async_copy(bounce, bounce, sems.at[1]).wait()

    def put(j, _):
        b = other[blocks + j]
        pltpu.make_async_copy(bounce.at[j], out_hbm.at[b], sems.at[2]).start()
        return 0

    lax.fori_loop(0, blocks - touch, put, 0)
    pltpu.make_async_copy(bounce, bounce, sems.at[2]).wait()


def keep_untouched(touched, table):
    blocks, _, width = table.shape
    touch = touched.shape[1]
    return call(
        keep_kernel,
        4.0,
        60,
        out_shape=like(table.shape, table.dtype),
        in_specs=[HBM, HBM],
        out_specs=HBM,
        scratch_shapes=[
            pltpu.SMEM((1, touch), jnp.int32),
            pltpu.VMEM((blocks - touch, BLOCK, width), table.dtype),
            pltpu.SMEM((2 * blocks,), jnp.int32),
            pltpu.SemaphoreType.DMA((3,)),
        ],
    )(touched, table)


def slot_keys(slot_ref, slabs, slots):
    per = LANES // slots
    lane = lax.broadcasted_iota(jnp.int32, (1, LANES), 1)
    table = jnp.broadcast_to(slot_ref[0:1, :], (META, LANES))
    keys = []
    for ref, i in slabs:
        meta = ref[i, slots : slots + META, :].astype(jnp.float32).astype(jnp.int32)
        local = jnp.broadcast_to(meta[0:1, :], (META, LANES))
        slot = jnp.take_along_axis(table, local, axis=1)[0:1, :]
        keys.append(jnp.where(slot >= 0, slot * BLOCK + meta[1:2, :], -1))
    lines = []
    for g in range(len(slabs) // per):
        line = keys[g * per]
        for j in range(1, per):
            key = pltpu.roll(keys[g * per + j], j * slots, 1)
            line = jnp.where((lane >= j * slots) & (lane < (j + 1) * slots), key, line)
        lines.append(line)
    return lines


def add_rows(slots, count, fresh, last, slot_ref, *refs):
    data, refs = refs[:count], refs[count:]
    sums_ref, weights = refs[0 if fresh else 1], refs[-1]
    touch, _, width = sums_ref.shape
    per = TILE // slots
    slabs = [(ref, i) for ref in data for i in range(ref.shape[0])]
    tiles = len(slabs) // per
    many = next(m for m in (4, 2, 1) if touch % m == 0)
    lines = slot_keys(slot_ref, slabs, slots)
    key_rows = []
    for k in range(tiles):
        pair = lines[2 * k : 2 * k + 2]
        upper = [((key >> 7) & 1).astype(jnp.float32) for key in pair]
        upper = [jnp.broadcast_to(u, (LANES, LANES)).T for u in upper]
        upper = jnp.concatenate(upper, axis=0).astype(jnp.bfloat16)
        rows = [ref[i, 0:slots, :] for ref, i in slabs[k * per : (k + 1) * per]]
        rows = jnp.concatenate(rows, axis=0)
        high = rows * upper
        weights[k, :, width : 2 * width] = high
        weights[k, :, 0:width] = rows - high
        flat = [jnp.where(key >= 0, (key >> 8) * LANES + (key & (LANES - 1)), -1) for key in pair]
        key_rows.append(jnp.concatenate(flat, axis=1))
    row = lax.broadcasted_iota(jnp.int32, (many * LANES, TILE), 0)
    if last:
        own_lane = lax.broadcasted_iota(jnp.int32, (LANES, LANES), 0) == (
            lax.broadcasted_iota(jnp.int32, (LANES, LANES), 1)
        )
        mean_rep_ref, flat_ref, square_ref = refs[2:5]

    def step(u, carry):
        total = None
        for k in range(tiles):
            match = row == jnp.broadcast_to(key_rows[k] - u * (many * LANES), row.shape)
            onehot = jnp.where(match, 1.0, 0.0).astype(jnp.bfloat16)
            part = jnp.dot(onehot, weights[k], preferred_element_type=jnp.float32)
            total = part if total is None else total + part
        for i in range(many):
            t = u * many + i
            for p in range(PARTS):
                piece = total[i * LANES : (i + 1) * LANES, p * width : (p + 1) * width]
                at = pl.ds(p * LANES, LANES)
                piece = piece if fresh else piece + sums_ref[t, at, :]
                sums_ref[t, at, :] = piece
                if last:
                    mean = jnp.sum(piece * piece, axis=1, keepdims=True) * (1.0 / width)
                    mean = jnp.broadcast_to(mean, (LANES, LANES))
                    mean_rep_ref[t, at, :] = mean
                    line = jnp.sum(jnp.where(own_lane, mean, 0.0), axis=0, keepdims=True)
                    flat_ref[pl.ds(t * PARTS + p, 1), :] = line
        return carry

    lax.fori_loop(0, touch // many, step, 0)
    if last:
        square = jnp.sum(flat_ref[...].reshape(-1, 8, LANES), axis=0) * width
        for i in range(square_ref.shape[0]):
            square_ref[i] = square


def sums_of(slot, data, slots, touch, sums=None, shards=0):
    width = data[0].shape[-1]
    count = len(data)
    slabs = sum(each.shape[0] for each in data)
    fresh, last = sums is None, shards > 0
    assert slabs * slots % TILE == 0 and touch * PARTS % 8 == 0
    outs = (like((touch, BLOCK, width)),)
    if last:
        outs += (
            like((touch, BLOCK, LANES)),
            like((touch * PARTS, LANES)),
            like((shards, 8, LANES)),
        )
    return call(
        functools.partial(add_rows, slots, count, fresh, last),
        slabs * slots / 512,
        10,
        out_shape=outs,
        in_specs=[VMEM] * (1 + count + (not fresh)),
        out_specs=(VMEM,) * len(outs),
        scratch_shapes=[pltpu.VMEM((slabs * slots // TILE, TILE, 2 * width), data[0].dtype)],
        input_output_aliases={} if fresh else {1 + count: 0},
    )(slot, *data, *([] if fresh else [sums]))


def spread_kernel(touched_hbm, accum_hbm, rep_ref, slot_ref, listed, accum, sems):
    a = pltpu.make_async_copy(touched_hbm, listed, sems.at[0])
    b = pltpu.make_async_copy(accum_hbm, accum, sems.at[1])
    a.start()
    b.start()
    a.wait()
    b.wait()
    lane = lax.broadcasted_iota(jnp.int32, slot_ref.shape, 1)

    def step(t, slot):
        block = listed[0, t]
        for part in range(PARTS):
            row = accum[pl.ds(block * PARTS + part, 1), :]
            rep_ref[t, part * LANES : (part + 1) * LANES, :] = jnp.broadcast_to(
                row, (LANES, LANES)
            ).T
        return jnp.where(lane == block, t, slot)

    start = jnp.full(slot_ref.shape, -1, jnp.int32)
    slot_ref[...] = lax.fori_loop(0, rep_ref.shape[0], step, start)


def spread_accum(touched, accum):
    touch = touched.shape[1]
    return call(
        spread_kernel,
        2.0,
        8,
        out_shape=(like((touch, BLOCK, LANES)), like((8, LANES), jnp.int32)),
        in_specs=[HBM, HBM],
        out_specs=(VMEM, VMEM),
        scratch_shapes=[
            pltpu.SMEM((1, touch), jnp.int32),
            pltpu.VMEM(accum.shape, accum.dtype),
            pltpu.SemaphoreType.DMA((2,)),
        ],
    )(touched, accum)


def update_kernel(
    limit, touched_hbm, square_ref, sums_ref, table_ref, accum_rep_ref, mean_rep_ref,
    flat_ref, accum_hbm, table_in, out_hbm, new_accum_hbm, fresh, accum, listed, sems,
):
    fetch = pltpu.make_async_copy(touched_hbm, listed, sems.at[0])
    fetch_accum = pltpu.make_async_copy(accum_hbm, accum, sems.at[1])
    fetch.start()
    fetch_accum.start()
    touch = fresh.shape[0]
    square = jnp.sum(square_ref[...], axis=0)
    square = jnp.sum(jnp.sum(square, axis=1, keepdims=True), axis=0, keepdims=True)
    factor = limit / jnp.maximum(jnp.sqrt(square), limit)
    factor_sq = factor * factor
    rate = LEARN_RATE * factor
    fetch.wait()

    def step(t, _):
        b = listed[0, t]
        root = lax.rsqrt(accum_rep_ref[t] + factor_sq * mean_rep_ref[t])
        fresh[t] = table_ref[b] * (1.0 - DECAY_RATE) - (rate * sums_ref[t]) * root
        pltpu.make_async_copy(fresh.at[t], out_hbm.at[b], sems.at[2]).start()
        return 0

    fetch_accum.wait()
    for t in range(touch):
        for part in range(PARTS):
            at = pl.ds(listed[0, t] * PARTS + part, 1)
            j = t * PARTS + part
            accum[at, :] = accum[at, :] + factor_sq * flat_ref[j : j + 1, :]
    put = pltpu.make_async_copy(accum, new_accum_hbm, sems.at[3])
    put.start()
    lax.fori_loop(0, touch, step, 0)
    put.wait()
    pltpu.make_async_copy(fresh, fresh, sems.at[2]).wait()


def update(limit, touched, square, sums, table, accum_rep, mean_rep, flat, accum, table_out):
    return call(
        functools.partial(update_kernel, limit),
        2.5,
        8,
        out_shape=(like(table.shape, table.dtype), like(accum.shape, accum.dtype)),
        in_specs=[HBM] + [VMEM] * 6 + [HBM] * 2,
        out_specs=(HBM, HBM),
        scratch_shapes=[
            pltpu.VMEM(sums.shape, table.dtype),
            pltpu.VMEM(accum.shape, accum.dtype),
            pltpu.SMEM(touched.shape, jnp.int32),
            pltpu.SemaphoreType.DMA((4,)),
        ],
        input_output_aliases={8: 0},
    )(touched, square, sums, table, accum_rep, mean_rep, flat, accum, table_out)


def exchange(x):
    return lax.all_to_all(x, "shard", 0, 0, tiled=True)


def step(row_ids, grad_rows, touched, block_home, embed_table, row_accum):
    slots, width = grad_rows.shape[3:]
    blocks_here = embed_table.shape[0] // BLOCK
    touch = touched.shape[1]
    shards = lax.axis_size("shard")
    reps = lax.axis_size("rep")
    limit = CLIP_RMS * math.sqrt(shards * touch * BLOCK * width)
    ids, grads = row_ids[0, 0], grad_rows[0, 0]
    table = embed_table.reshape(blocks_here, BLOCK, width)
    accum = row_accum.reshape(-1, LANES)
    home = jnp.pad(block_home, (0, -block_home.shape[0] % LANES)).reshape(-1, LANES)
    direct = EARLY if shards > EARLY and EARLY * slots >= TILE else 0

    def swap(x, r=0):
        pairs = [
            (rep * shards + i, (rep + 1) % reps * shards + (i ^ r))
            for rep in range(reps)
            for i in range(shards)
        ]
        return lax.ppermute(x, ("rep", "shard"), pairs)

    data, *early = pack(ids, home, grads, blocks_here, direct)
    data = exchange(data)
    early = [swap(each, r) for r, each in enumerate(early)]
    table_out = keep_untouched(touched, table)
    accum_rep, slot = spread_accum(touched, accum)
    if direct:
        far_a, far_b = pick_far(data, direct)
    else:
        far_a, far_b = data[: shards // 2], data[shards // 2 :]
    far_a = swap(far_a)
    far_b = swap(far_b)
    (sums,) = sums_of(slot, [data, *early], slots, touch)
    (sums,) = sums_of(slot, [far_a], slots, touch, sums)
    sums, mean_rep, flat, square = sums_of(slot, [far_b], slots, touch, sums, shards)
    square = exchange(square)
    table_out, accum_out = update(
        limit, touched, square, sums, table, accum_rep, mean_rep, flat, accum, table_out
    )
    return table_out.reshape(-1, width), accum_out.reshape(-1)


def solution(mesh):
    shards = mesh.shape["shard"]
    assert mesh.shape["rep"] == 2 and shards & (shards - 1) == 0
    in_specs = (
        P("rep", "shard", None, None),
        P("rep", "shard", None, None, None),
        P("shard", None),
        P(),
        P("shard", None),
        P("shard"),
    )
    out_specs = (P("shard", None), P("shard"))
    return jax.shard_map(step, mesh=mesh, in_specs=in_specs, out_specs=out_specs, check_vma=False)
```
